256 devices in a mesh: occ: 64 (over z, y, core), ao: 4 (over x).
Axes of the slice: x: 4, y: 4, z: 8, core: 2. Of those that a mesh axis runs over, the one named last changes fastest.
Arguments:
- amplitudes: bfloat16 [8, 5120, 19456], P(None, 'occ', 'ao'), may hold values from -6 to 6
- occ_coef: bfloat16 [512, 5120], P(None, 'occ'), may hold values from -0.25 to 0.25
- vir_coef: bfloat16 [512, 19456], P('occ', 'ao'), may hold values from -0.25 to 0.25
- occ_energy: float32 [5120], P('occ'), may hold values from -1.5 to -0.3
- vir_energy: float32 [19456], P('ao'), may hold values from 0.05 to 2.5
- kernel: float32 [512], replicated, may hold values from 2 to 10
Outputs:
- residual: bfloat16 [8, 5120, 19456], P(None, 'occ', 'ao')
- projected: float32 [8, 8], replicated
The draws below stay inside these ranges and needn't reach their ends.
All inputs are finite; a program needn't handle non-finite values.
Results may differ from the reference program's by a relative error of at most 0.0049.
Values may be sent and summed in bfloat16 or wider, within the bound.
A program may use at most 128 MiB of HBM per device.

```python
import math
import jax
import jax.numpy as jnp
from jax import lax

K = 8
NVIR = 19456
ROWS = 512
NOCC = 5120


def level_of(own_key, shape, cuts, smallest, high):
    factor_of, own = 1.0, jax.random.fold_in(own_key, 6)
    for position, shards_of in cuts:
        draws = jnp.exp(jax.random.uniform(jax.random.fold_in(own, position), (shards_of,), jnp.float32, smallest / len(cuts), high / len(cuts)))
        factor_of = factor_of * jnp.repeat(draws, shape[position] // shards_of).reshape([-1 if axis == position else 1 for axis in range(len(shape))])
    return factor_of


def bell_draw(key, shape, deviation, limit, pieces=(), dtype=jnp.bfloat16):
    array = jax.random.normal(key, shape, jnp.float32) * deviation
    if len(pieces) > 0:
        array = level_of(key, shape, pieces, -0.22, 0.18) * array
    return jnp.clip(array, min=-limit, max=limit).astype(dtype)


def setup_inputs(seed: int = 0) -> dict:
    splits = jax.random.split(jax.random.key(seed), 7)
    amplitudes = bell_draw(splits[0], (K, NOCC, NVIR), 1.0, 6.0, ((1, 64), (2, 4)))
    occ_coef = bell_draw(splits[1], (ROWS, NOCC), ROWS ** -0.5, 0.25, ((1, 64),))
    vir_coef = bell_draw(splits[2], (ROWS, NVIR), ROWS ** -0.5, 0.25, ((0, 64), (1, 4)))
    occ_energy = jnp.clip(-1.5 + 1.2 * jax.random.uniform(splits[3], (NOCC,), jnp.float32) ** level_of(splits[3], (NOCC,), ((0, 64),), -0.2, 0.2), -1.5, -0.3)
    vir_energy = jnp.clip(0.05 + 2.45 * jax.random.uniform(splits[4], (NVIR,), jnp.float32) ** level_of(splits[4], (NVIR,), ((0, 4),), -0.2, 0.2), 0.05, 2.5)
    kernel = jnp.clip(jnp.exp(jax.random.uniform(splits[5], (ROWS,), jnp.float32, math.log(2.0), math.log(10.0))), 2.0, 10.0)
    return {"amplitudes": amplitudes, "occ_coef": occ_coef, "vir_coef": vir_coef, "occ_energy": occ_energy, "vir_energy": vir_energy, "kernel": kernel}


def reference(amplitudes, occ_coef, vir_coef, occ_energy, vir_energy, kernel):
    occ_float = occ_coef.astype(jnp.float32)
    energy_gaps = vir_energy[None, :] - occ_energy[:, None]

    def sigma_of(trial_amps):
        half_done = jnp.dot(trial_amps, vir_coef.T, preferred_element_type=jnp.float32)
        density = lax.optimization_barrier(jnp.sum(occ_float.T * half_done, axis=0))
        potential = kernel * density
        weighted = (occ_float * potential[:, None]).astype(jnp.bfloat16)
        coupling = jnp.dot(weighted.T, vir_coef, preferred_element_type=jnp.float32)
        return energy_gaps * trial_amps.astype(jnp.float32) + coupling
    sigma_all = lax.map(sigma_of, amplitudes)
    flat_amps = amplitudes.reshape(K, -1)
    correlation = jnp.dot(flat_amps, flat_amps.T, preferred_element_type=jnp.float32)

    def gram_column(sigma_one):

        def one_entry(trial_amps):
            return jnp.sum(trial_amps.astype(jnp.float32) * sigma_one)
        return lax.map(one_entry, amplitudes)
    gram = lax.map(gram_column, sigma_all).T
    norms = jnp.diagonal(correlation) + 1e-06
    ritz_values = jnp.diagonal(gram) / norms
    residual = (sigma_all - ritz_values[:, None, None] * amplitudes.astype(jnp.float32)).astype(jnp.bfloat16)
    projected = gram / jnp.sqrt(norms[:, None] * norms[None, :])
    return (residual, projected)
```

```python
import jax
import jax.numpy as jnp
from jax import lax
from jax.sharding import Mesh
from jax.sharding import PartitionSpec as P

OCC = ("occ_0", "occ_1", "occ_2")


def laid_out(tiles, dim):
    tiles = jnp.moveaxis(tiles, 0, dim)
    dims = tiles.shape
    return tiles.reshape(*dims[:dim], dims[dim] * dims[dim + 1], *dims[dim + 2 :])


def stacked_from(x, axes, order):
    tiles = x
    for k in order:
        tiles = lax.all_gather(tiles, axes[k])
    done = order[::-1]
    back = [done.index(k) for k in range(len(axes))]
    tiles = tiles.transpose(*back, *range(len(axes), tiles.ndim))
    return tiles.reshape(-1, *x.shape)


def gather_axes(x, axes, order, dim):
    return laid_out(stacked_from(x, axes, order), dim)


def sent_to_all(x, axis):
    copies = jnp.broadcast_to(x, (lax.axis_size(axis), *x.shape))
    return lax.all_to_all(copies, axis, split_axis=0, concat_axis=0, tiled=True)


def over_copies(x, axis):
    everything = sent_to_all(x, axis)
    return jnp.sum(everything, axis=0)


def one_axis_at_a_time(x, axes):
    far, near = axes
    return over_copies(over_copies(x, near), far)


def packed_total(arrays, axis):
    vector, at, finished = (jnp.concatenate([a.reshape(-1) for a in arrays]), 0, [])
    running = one_axis_at_a_time(vector, axis)
    for a in arrays:
        finished.append(running[at : at + a.size].reshape(a.shape))
        at += a.size
    return tuple(finished)


def shards(amplitudes, occ_coef, vir_coef, occ_energy, vir_energy, kernel):
    trials, occ_dev, vir_dev = amplitudes.shape
    row_total = occ_coef.shape[0]
    flat_amps = amplitudes.reshape(trials * occ_dev, vir_dev)
    occ_trans = occ_coef.T.astype(jnp.float32)
    energy_gaps = vir_energy[None, :] - occ_energy[:, None]
    amps_rows = amplitudes.reshape(trials, occ_dev * vir_dev)
    gap_rows = (energy_gaps[None] * amplitudes.astype(jnp.float32)).astype(jnp.bfloat16)
    gap_rows = gap_rows.reshape(trials, occ_dev * vir_dev)
    correlation_local = jnp.dot(amps_rows, amps_rows.T, preferred_element_type=jnp.float32)
    gap_local = jnp.dot(amps_rows, gap_rows.T, preferred_element_type=jnp.float32)
    whole_rows = gather_axes(vir_coef, OCC, (1, 0, 2), 0)
    row_count = whole_rows.shape[0]
    half_done = lax.dot_general(
        flat_amps, whole_rows, (((1,), (1,)), ((), ())), preferred_element_type=jnp.float32
    )
    half_done = half_done.reshape(trials, occ_dev, row_count)
    partial_value = jnp.sum(half_done * occ_trans[None], axis=1)
    density, correlation, gap_gram = packed_total(
        (partial_value, correlation_local, gap_local), ("occ_0", ("occ_1", "occ_2", "ao"))
    )
    potential = kernel[None, :] * density
    gram = gap_gram + jnp.sum(density[:, None, :] * potential[None, :, :], axis=-1)
    norms = jnp.diagonal(correlation) + 1e-06
    ritz_values = jnp.diagonal(gram) / norms
    weighted = (
        (occ_trans[None] * potential[:, None, :])
        .astype(jnp.bfloat16)
        .reshape(trials * occ_dev, row_total)
    )
    coupling = jnp.dot(weighted, whole_rows, preferred_element_type=jnp.float32)
    shifted = energy_gaps[None] - ritz_values[:, None, None]
    residual = (
        shifted * amplitudes.astype(jnp.float32) + coupling.reshape(trials, occ_dev, vir_dev)
    ).astype(jnp.bfloat16)
    projected = gram / jnp.sqrt(norms[:, None] * norms[None, :])
    return (residual, projected)


def solution(mesh):
    torus = Mesh(mesh.devices.reshape(8, 4, 2, mesh.shape["ao"]), ("occ_0", "occ_1", "occ_2", "ao"))
    in_specs = (P(None, OCC, "ao"), P(None, OCC), P(OCC, "ao"), P(OCC), P("ao"), P())
    out_specs = (P(None, OCC, "ao"), P())
    return jax.shard_map(
        shards, mesh=torus, in_specs=in_specs, out_specs=out_specs, check_vma=False
    )
```

```python
import functools

import jax
import jax.numpy as jnp
from jax import lax
from jax.experimental import pallas as pl
from jax.experimental.pallas import tpu as pltpu
from jax.sharding import PartitionSpec as P

F32 = jnp.float32
BF16 = jnp.bfloat16
MESH = pl.DeviceIdType.MESH
NZ, NY, NC, NX = 8, 4, 2, 4
K, I, M, A = 8, 80, 512, 4864
FIRST = (0, 2048)
SECOND = (2048, 4864)
PARTS = (FIRST, SECOND)
EXTRA = 128
WIDE = M + EXTRA
SLICES = ((0, 1024), (1024, 2048), (2048, 3072), (3072, 4096), (4096, 4864))
AMP_CUTS = ((0, 1280), (1280, 2560), (2560, 3840), (3840, 4864))


def signed(d, n):
    return d if d <= n // 2 else d - n


def columns_of(part, half):
    low, high = PARTS[part]
    middle = (low + high) // 2
    return {None: (low, high), 0: (low, middle), 1: (middle, high)}[half]


def onward(part, half, dy, dz):
    sy, sz = signed(dy, NY), signed(dz, NZ)
    out = []
    if part == 0:
        if sz == 0:
            if sy == 0:
                out += [(None, 1, 0), (None, -1, 0)]
            elif sy == -1:
                out.append((0, 1, 0))
            elif sy == 1:
                out.append((1, -1, 0))
            out += [(None, 0, 1), (None, 0, -1)]
        elif sz in (-1, -2):
            out.append((None, 0, 1))
        elif sz == -3:
            out.append((0, 0, 1))
        elif sz in (1, 2):
            out.append((None, 0, -1))
        elif sz == 3:
            out.append((1, 0, -1))
    else:
        if sy == 0:
            if sz in (0, -1, -2):
                out.append((None, 0, 1))
            if sz in (0, 1, 2):
                out.append((None, 0, -1))
            if sz == -3:
                out.append((0, 0, 1))
            if sz == 3:
                out.append((1, 0, -1))
            out += [(None, 1, 0), (None, -1, 0)]
        elif sy == -1:
            out.append((0, 1, 0))
        elif sy == 1:
            out.append((1, -1, 0))
    return out


def halves_of(part, dy, dz):
    sy, sz = signed(dy, NY), signed(dz, NZ)
    if part == 0:
        split = sz == 4 or (sz == 0 and sy == 2)
    else:
        split = sy == 2 or (sy == 0 and sz == 4)
    return (0, 1) if split else (None,)


LEVELS = [
    [
        (part, dy, dz)
        for dz in (0, 7, 1, 6, 2, 5, 3, 4)
        for dy in (0, 3, 1, 2)
        for part in (1, 0)
        if abs(signed(dy, NY)) + abs(signed(dz, NZ)) == level
    ]
    for level in range(7)
]


def gather_kernel(
    vir_ref,
    amps_ref,
    occ_ref,
    occ_e_ref,
    vir_e_ref,
    rows_ref,
    amps_out,
    total_ref,
    half_acc,
    corr_acc,
    gap_acc,
    za,
    ya,
    xa,
    link_send,
    link_recv,
    pair_send,
    pair_recv,
    local_sem,
    amp_sem,
    z_send,
    z_recv,
    y_send,
    y_recv,
    x_send,
    x_recv,
):
    me = lax.axis_index("occ")
    x = lax.axis_index("ao")
    z, y, c = me // (NY * NC), (me // NC) % NY, me % NC

    def at(zz, yy, cc):
        return lax.rem(zz + 2 * NZ, NZ) * (NY * NC) + lax.rem(yy + 2 * NY, NY) * NC + cc

    barrier = pltpu.get_barrier_semaphore()
    near = [(at(z, y + 1, c), x), (at(z, y - 1, c), x), (at(z + 1, y, c), x), (at(z - 1, y, c), x)]
    near.append((at(z, y, 1 - c), x))
    near += [(me, lax.rem(x + d, NX)) for d in (1, 2, 3)]
    for device in near:
        pl.semaphore_signal(barrier, inc=1, device_id=device, device_id_type=MESH)

    def rows_at(dy, dz, cc):
        start = pl.multiple_of(at(z + signed(dz, NZ), y + signed(dy, NY), cc) * 8, 8)
        return pl.ds(start, 8)

    own = pltpu.make_async_copy(vir_ref, rows_ref.at[rows_at(0, 0, c), :], local_sem)
    own.start()
    amp_copies = []
    for n, (low, high) in enumerate(AMP_CUTS):
        amp_copies.append(
            pltpu.make_async_copy(
                amps_ref.at[:, pl.ds(low, high - low)],
                amps_out.at[:, pl.ds(low, high - low)],
                amp_sem.at[n],
            )
        )
    for copy in amp_copies:
        copy.start()
    own.wait()
    pl.semaphore_wait(barrier, len(near))

    sent = []

    def piece(part, half, dy, dz, cc):
        low, high = columns_of(part, half)
        return rows_ref.at[rows_at(dy, dz, cc), pl.ds(low, high - low)]

    def recv_index(part, half, dy, dz):
        return ((part * 2 + (half or 0)) * NY + dy) * NZ + dz

    def link_copy(part, half, dy, dz, step_y, step_z):
        block = piece(part, half, dy, dz, c)
        return pltpu.make_async_remote_copy(
            src_ref=block,
            dst_ref=block,
            send_sem=link_send.at[len(sent)],
            recv_sem=link_recv.at[
                recv_index(part, half, (dy - step_y) % NY, (dz - step_z) % NZ)
            ],
            device_id=(at(z + step_z, y + step_y, c), x),
            device_id_type=MESH,
        )

    def arrival(part, half, dy, dz):
        block = piece(part, half, dy, dz, c)
        return pltpu.make_async_copy(block, block, link_recv.at[recv_index(part, half, dy, dz)])

    def pair_copy(part, dy, dz):
        block = piece(part, None, dy, dz, c)
        index = (part * NY + dy) * NZ + dz
        return pltpu.make_async_remote_copy(
            src_ref=block,
            dst_ref=block,
            send_sem=pair_send.at[index],
            recv_sem=pair_recv.at[index],
            device_id=(at(z, y, 1 - c), x),
            device_id_type=MESH,
        )

    pair_copies = []

    def pass_on(part, dy, dz):
        for half, step_y, step_z in onward(part, None, dy, dz):
            copy = link_copy(part, half, dy, dz, step_y, step_z)
            copy.start()
            sent.append(copy)
        copy = pair_copy(part, dy, dz)
        copy.start()
        pair_copies.append(copy)

    def receive(part, dy, dz):
        for half in halves_of(part, dy, dz):
            arrival(part, half, dy, dz).wait()
        pass_on(part, dy, dz)

    def pair_arrival(part, dy, dz):
        block = piece(part, None, dy, dz, 1 - c)
        pltpu.make_async_copy(
            block, block, pair_recv.at[(part * NY + dy) * NZ + dz]
        ).wait()

    square = (lax.broadcasted_iota(jnp.int32, (I, I), 0), lax.broadcasted_iota(jnp.int32, (I, I), 1))
    occ_e = jnp.sum(
        jnp.where(square[0] == square[1], jnp.broadcast_to(occ_e_ref[...], (I, I)), 0.0),
        axis=1,
        keepdims=True,
    )

    def trial_sums(block):
        corr = jnp.zeros((128, 128), F32)
        gaps = jnp.zeros((128, 128), F32)
        for low, high in SLICES:
            rows = [amps_out[k * I + block * 16 : k * I + block * 16 + 16, low:high] for k in range(K)]
            chunk = jnp.concatenate(rows, axis=0)
            scaled = (chunk.astype(F32) * vir_e_ref[:, low:high]).astype(BF16)
            dims = (((1,), (1,)), ((), ()))
            corr += lax.dot_general(chunk, chunk, dims, preferred_element_type=F32)
            gaps += lax.dot_general(chunk, scaled, dims, preferred_element_type=F32)
        levels = jnp.concatenate([occ_e[block * 16 : block * 16 + 16]] * K, axis=0)
        gaps -= levels * corr
        if block == 0:
            corr_acc[...] = corr
            gap_acc[...] = gaps
        else:
            corr_acc[...] += corr
            gap_acc[...] += gaps

    def trial_totals():
        r = lax.broadcasted_iota(jnp.int32, (128, 128), 0)
        q = lax.broadcasted_iota(jnp.int32, (128, 128), 1)
        same = (r % 16) == (q % 16)
        pick = lax.broadcasted_iota(jnp.int32, (128, EXTRA), 0) // 16
        lane = lax.broadcasted_iota(jnp.int32, (128, EXTRA), 1)
        out = jnp.zeros((K, EXTRA), F32)
        for n, acc in enumerate((corr_acc, gap_acc)):
            kept = jnp.where(same, acc[...], 0.0)
            summed = jnp.sum(kept.reshape(K, 16, 128), axis=1)
            chosen = (pick + n * K == lane).astype(F32)
            out += jnp.dot(
                summed, chosen, precision=lax.Precision.HIGHEST, preferred_element_type=F32
            )
        return out

    def half_done(group, low, high):
        rows = []
        for n in range(4):
            start = lax.rem(z + NZ - 2 + group * 4 + n, NZ) * 64
            rows.append(rows_ref[pl.ds(pl.multiple_of(start, 64), 64), low:high])
        vir = jnp.concatenate(rows, axis=0)
        part = lax.dot_general(
            amps_out[:, low:high], vir, (((1,), (1,)), ((), ())), preferred_element_type=F32
        )
        if low == 0:
            half_acc[...] = part
        else:
            half_acc[...] += part

    turn = lax.rem(z + NZ - 2, NZ) * 64
    occ_rel = pltpu.roll(occ_ref[...].astype(F32), lax.rem(M - turn, M), 1)

    def partial_density(group):
        occ = occ_rel[:, group * 256 : group * 256 + 256]
        rows = []
        for k in range(K):
            rows.append(jnp.sum(half_acc[k * I : k * I + I, :] * occ, axis=0, keepdims=True))
        return jnp.concatenate(rows, axis=0)

    for part, dy, dz in LEVELS[0]:
        pass_on(part, dy, dz)
    for copy in amp_copies:
        copy.wait()
    trial_sums(0)
    trial_sums(1)
    for step in LEVELS[1]:
        receive(*step)
    trial_sums(2)
    for step in LEVELS[2]:
        receive(*step)
    trial_sums(3)
    for step in LEVELS[3]:
        receive(*step)
    trial_sums(4)
    extra = trial_totals()
    for step in LEVELS[4]:
        receive(*step)
    early = [(p, dy, dz) for p in (0, 1) for dy in range(NY) for dz in (6, 7, 0, 1)]
    late = [(p, dy, dz) for p in (0, 1) for dy in range(NY) for dz in (2, 3, 4, 5)]
    for step in early:
        pair_arrival(*step)
    half_done(0, *SLICES[0])
    half_done(0, *SLICES[1])
    for step in LEVELS[5]:
        receive(*step)
    for cut in SLICES[2:]:
        half_done(0, *cut)
    first = partial_density(0)
    for step in LEVELS[6]:
        receive(*step)
    for step in late:
        pair_arrival(*step)
    for cut in SLICES:
        half_done(1, *cut)
    second = partial_density(1)
    density = pltpu.roll(jnp.concatenate([first, second], axis=1), turn, 1)

    def all_sum(slots, mine, count, send, recv, device_of):
        copies = []
        for d in range(1, count):
            copies.append(
                pltpu.make_async_remote_copy(
                    src_ref=slots.at[mine],
                    dst_ref=slots.at[mine],
                    send_sem=send.at[d],
                    recv_sem=recv.at[(count - d) % count],
                    device_id=device_of(d),
                    device_id_type=MESH,
                )
            )
        for copy in copies:
            copy.start()
        for d in range(1, count):
            other = slots.at[lax.rem(mine + d, count)]
            pltpu.make_async_copy(other, other, recv.at[d]).wait()
        out = slots[0]
        for n in range(1, count):
            out = out + slots[n]
        return out, copies

    za[z, :, :M] = density
    za[z, :, M:] = extra
    total, z_copies = all_sum(
        za, z, NZ, z_send, z_recv, lambda d: (at(z + d, y, c), x)
    )
    place = y * NC + c
    ya[place] = total
    total, y_copies = all_sum(
        ya,
        place,
        NY * NC,
        y_send,
        y_recv,
        lambda d: (z * (NY * NC) + lax.rem(place + d, NY * NC), x),
    )
    xa[x] = total
    total, x_copies = all_sum(
        xa, x, NX, x_send, x_recv, lambda d: (me, lax.rem(x + d, NX))
    )
    total_ref[...] = total
    for copy in sent + pair_copies + z_copies + y_copies + x_copies:
        copy.wait_send()


SENDS = sum(
    len(onward(part, None, dy, dz)) for level in LEVELS for part, dy, dz in level
)
BLOCKS = [(n * 256, n * 256 + 256) for n in range(A // 256)]


def residual_kernel(
    rows_ref,
    amps_ref,
    total_ref,
    occ_ref,
    occ_e_ref,
    vir_e_ref,
    kernel_ref,
    out_ref,
    projected_ref,
    weighted,
    staged,
    out_sem,
):
    density = total_ref[:, :M]
    correlation = total_ref[:, M : M + K]
    gap_gram = total_ref[:, M + K : M + 2 * K]
    potential = kernel_ref[...] * density
    occ = occ_ref[...].astype(F32)
    for k in range(K):
        weighted[k * I : k * I + I, :] = (occ * potential[k : k + 1, :]).astype(BF16)
    lane = lax.broadcasted_iota(jnp.int32, (K, K), 1)
    row = lax.broadcasted_iota(jnp.int32, (K, K), 0)
    gram = gap_gram
    for m in range(K):
        column = jnp.sum(density * potential[m : m + 1, :], axis=1, keepdims=True)
        gram = gram + jnp.where(lane == m, column, 0.0)
    diagonal = lane == row
    kept = jnp.where(diagonal, correlation, 0.0)
    norm_col = jnp.sum(kept, axis=1, keepdims=True) + 1e-6
    norm_row = jnp.sum(kept, axis=0, keepdims=True) + 1e-6
    projected_ref[...] = gram / jnp.sqrt(norm_col * norm_row)
    ritz = jnp.sum(jnp.where(diagonal, gram, 0.0), axis=1, keepdims=True) / norm_col
    square = (lax.broadcasted_iota(jnp.int32, (I, I), 0), lax.broadcasted_iota(jnp.int32, (I, I), 1))
    occ_e = jnp.sum(
        jnp.where(square[0] == square[1], jnp.broadcast_to(occ_e_ref[...], (I, I)), 0.0),
        axis=1,
        keepdims=True,
    )
    copies = []
    for n, (low, high) in enumerate(BLOCKS):
        coupling = jnp.dot(weighted[...], rows_ref[:, low:high], preferred_element_type=F32)
        for k in range(K):
            shift = occ_e + ritz[k : k + 1, :]
            gaps = vir_e_ref[:, low:high] - shift
            rows = slice(k * I, k * I + I)
            staged[rows, low:high] = (
                gaps * amps_ref[rows, low:high].astype(F32) + coupling[rows]
            ).astype(BF16)
        copy = pltpu.make_async_copy(
            staged.at[:, pl.ds(low, high - low)], out_ref.at[:, pl.ds(low, high - low)], out_sem.at[n]
        )
        copy.start()
        copies.append(copy)
    for copy in copies:
        copy.wait()


def shards(amplitudes, occ_coef, vir_coef, occ_energy, vir_energy, kernel):
    amps = amplitudes.reshape(K * I, A)
    occ = occ_coef.T
    occ_e = occ_energy.reshape(1, I)
    vir_e = vir_energy.reshape(1, A)
    vmem = pl.BlockSpec(memory_space=pltpu.VMEM)
    hbm = pl.BlockSpec(memory_space=pl.ANY)
    dma = pltpu.SemaphoreType.DMA
    rows, amps_in, total = pl.pallas_call(
        gather_kernel,
        out_shape=(
            pltpu.VMEM((M, A), BF16),
            pltpu.VMEM((K * I, A), BF16),
            pltpu.VMEM((K, WIDE), F32),
        ),
        in_specs=[hbm, hbm, vmem, vmem, vmem],
        out_specs=(vmem, vmem, vmem),
        scratch_shapes=[
            pltpu.VMEM((K * I, 256), F32),
            pltpu.VMEM((128, 128), F32),
            pltpu.VMEM((128, 128), F32),
            pltpu.VMEM((NZ, K, WIDE), F32),
            pltpu.VMEM((NY * NC, K, WIDE), F32),
            pltpu.VMEM((NX, K, WIDE), F32),
            dma((SENDS,)),
            dma((2 * 2 * NY * NZ,)),
            dma((2 * NY * NZ,)),
            dma((2 * NY * NZ,)),
            dma,
            dma((len(AMP_CUTS),)),
            dma((NZ,)),
            dma((NZ,)),
            dma((NY * NC,)),
            dma((NY * NC,)),
            dma((NX,)),
            dma((NX,)),
        ],
        compiler_params=pltpu.CompilerParams(
            collective_id=0, has_side_effects=True, vmem_limit_bytes=20 * 2**20
        ),
        name="gather_and_reduce",
    )(vir_coef, amps, occ, occ_e, vir_e)
    residual, projected = pl.pallas_call(
        residual_kernel,
        out_shape=(
            jax.ShapeDtypeStruct((K * I, A), BF16),
            jax.ShapeDtypeStruct((K, K), F32),
        ),
        in_specs=[vmem] * 7,
        out_specs=(hbm, vmem),
        scratch_shapes=[
            pltpu.VMEM((K * I, M), BF16),
            pltpu.VMEM((K * I, A), BF16),
            dma((len(BLOCKS),)),
        ],
        compiler_params=pltpu.CompilerParams(vmem_limit_bytes=20 * 2**20),
        name="residual",
    )(rows, amps_in, total, occ, occ_e, vir_e, kernel.reshape(1, M))
    return residual.reshape(K, I, A), projected


def solution(mesh):
    in_specs = (P(None, "occ", "ao"), P(None, "occ"), P("occ", "ao"), P("occ"), P("ao"), P())
    out_specs = (P(None, "occ", "ao"), P())
    return jax.shard_map(
        shards, mesh=mesh, in_specs=in_specs, out_specs=out_specs, check_vma=False
    )
```
